32 devices in a mesh: gx: 16 (over z, x, core), gy: 2 (over y).
Axes of the slice: x: 2, y: 2, z: 4, core: 2. Of those that a mesh axis runs over, the one named last changes fastest.
Arguments:
- volt: float32 [128, 128, 2048], P('gx', 'gy'), may hold values from -6 to 6
- drive: float32 [128, 128, 2048], P('gx', 'gy'), may hold values from -6 to 6
- region: int32 [128, 128, 32], P('gx', 'gy'), may hold values from 0 to 7
- diode_mask: int32 [128, 128, 32], P('gx', 'gy'), may hold values 0 or 1
- sigma_table: float32 [8], replicated, may hold values from 0.3 to 3
- cap_table: float32 [8], replicated, may hold values from 0.1 to 1
Outputs:
- residual: float32 [128, 128, 2048], P('gx', 'gy')
- coef_norms: float32 [64], replicated
The draws below stay inside these ranges and needn't reach their ends.
All inputs are finite; a program needn't handle non-finite values. No bound on the sum of `diode_mask` on one device may be relied on, other than what follows from the above.
Results may differ from the reference program's by a relative error of at most 0.0003.
Values sent between devices are 32-bit elements; how exact they have to be, the bound alone decides.
A program may use at most 192 MiB of HBM per device.

```python
import math
import jax
import jax.numpy as jnp
from jax import lax

NZ = 32
H = 32
KC = 64
S = 256
REGIONS = 8
NX = 128
NY = 128


def with_ends(values, key, least, high):
    extent = values.shape
    place = [jax.random.randint(jax.random.fold_in(key, axis), (), 0, extent[axis]) for axis in range(len(extent))]
    values = values.at[tuple(place)].set(least)
    longest = extent.index(max(extent))
    place[longest] = (place[longest] + 1) % extent[longest]
    return values.at[tuple(place)].set(high)


def shard_levels(rng, shape, shards, least, high):
    def one(dim, shards_of):
        draws = jax.random.uniform(jax.random.fold_in(jax.random.fold_in(rng, 6), dim), (shards_of,), jnp.float32, least / len(shards), high / len(shards))
        return jnp.repeat(jnp.exp(draws), shape[dim] // shards_of).reshape((-1,) + (1,) * (len(shape) - dim - 1))

    loudness = one(*shards[0])
    for cut in shards[1:]:
        loudness = loudness * one(*cut)
    return loudness


def noise(stream_key, shape, spread, bound, pieces=(), held_as=jnp.bfloat16):
    gain = shard_levels(stream_key, shape, pieces, -0.22, 0.18) if pieces else 1.0
    entries = jax.random.normal(stream_key, shape, jnp.float32) * spread * gain
    return jnp.minimum(jnp.maximum(entries, -bound), bound).astype(held_as)


def setup_inputs(seed: int = 0) -> dict:
    key_of = jax.random.split(jax.random.key(seed), 7)
    return {
        "volt": noise(key_of[0], (NX, NY, NZ * KC), 1.0, 6.0, ((0, 16), (1, 2)), jnp.float32),
        "drive": noise(key_of[1], (NX, NY, NZ * KC), 1.0, 6.0, ((0, 16), (1, 2)), jnp.float32),
        "region": with_ends(jax.random.randint(key_of[2], (NX, NY, NZ), 0, REGIONS), jax.random.fold_in(key_of[2], 1), 0, REGIONS - 1).astype(jnp.int32),
        "diode_mask": with_ends((jax.random.randint(key_of[3], (NX, NY, NZ), 0, 4) < 1).astype(jnp.int32), jax.random.fold_in(key_of[3], 1), 0, 1),
        "sigma_table": jnp.clip(jnp.exp(jax.random.uniform(key_of[4], (REGIONS,), jnp.float32, math.log(0.3), math.log(3.0))), 0.3, 3.0),
        "cap_table": jnp.clip(jnp.exp(jax.random.uniform(key_of[5], (REGIONS,), jnp.float32, math.log(0.1), math.log(1.0))), 0.1, 1.0),
    }


base_freq = 0.1
norm_eps = 1e-06

def cut_slab(array, first_idx, last_idx, along):
    return lax.slice_in_dim(array, first_idx, last_idx, axis=along)

def harmonic_mean(left, right):
    return 2.0 * left * right / (left + right)

def open_terms(volt_field, conduct, along):
    cell_count = volt_field.shape[along]
    widths = [(0, 0)] * volt_field.ndim
    widths[along] = (1, 1)
    padded_volt = jnp.pad(volt_field, widths)
    padded_cond = jnp.pad(conduct, widths)
    face_flux = harmonic_mean(cut_slab(padded_cond, 0, cell_count + 1, along), cut_slab(padded_cond, 1, cell_count + 2, along)) * (cut_slab(padded_volt, 1, cell_count + 2, along) - cut_slab(padded_volt, 0, cell_count + 1, along))
    return cut_slab(face_flux, 0, cell_count, along) - cut_slab(face_flux, 1, cell_count + 1, along)

def time_derivative(coefs):
    half_count = coefs.shape[-1] // 2
    orders = base_freq * jnp.arange(1, half_count + 1, dtype=jnp.float32)
    return jnp.concatenate([orders * coefs[..., half_count:], -orders * coefs[..., :half_count]], axis=-1)

def spectral_tables(harmonics, samples):
    orders = jnp.arange(1, harmonics + 1, dtype=jnp.float32)
    times = 2.0 * math.pi * jnp.arange(samples, dtype=jnp.float32) / samples
    angles = orders[:, None] * times[None, :]
    synthesis = jnp.concatenate([jnp.cos(angles), jnp.sin(angles)], axis=0)
    analysis = synthesis.T * (2.0 / samples)
    return (synthesis, analysis)

def nonlinear_row(volt_row, diode_row, synthesis, analysis):
    coef_count = volt_row.shape[-1]
    flat = volt_row.reshape(-1, coef_count)
    cell_count = flat.shape[0]
    samples = jnp.dot(flat, synthesis, precision=lax.Precision.HIGHEST, preferred_element_type=jnp.float32)
    current = jax.nn.softplus(2.0 * samples) * 0.5
    charge = jnp.tanh(samples) * 0.5
    projected = jnp.dot(jnp.concatenate([current, charge], axis=0), analysis, precision=lax.Precision.HIGHEST, preferred_element_type=jnp.float32)
    combined = projected[:cell_count] + time_derivative(projected[cell_count:])
    return combined.reshape(volt_row.shape) * diode_row[..., None]

def reference(volt, drive, region, diode_mask, sigma_table, cap_table):
    conduct = jnp.take(sigma_table, region)[..., None]
    capacity = jnp.take(cap_table, region)[..., None]
    volt_field = volt.reshape(NX, NY, NZ, KC)
    drive_field = drive.reshape(NX, NY, NZ, KC)
    diode_field = diode_mask.astype(jnp.float32)
    synthesis, analysis = spectral_tables(H, S)

    def picker(array, row_index):
        return lax.dynamic_index_in_dim(array, row_index, 0, keepdims=False)

    def one_row(row_index):
        prev_row = (row_index - 1 + NX) % NX
        next_row = (row_index + 1) % NX
        volt_here = picker(volt_field, row_index)
        cond_here = picker(conduct, row_index)
        volt_prev = picker(volt_field, prev_row)
        cond_prev = picker(conduct, prev_row)
        volt_next = picker(volt_field, next_row)
        cond_next = picker(conduct, next_row)
        below_flux = harmonic_mean(cond_prev, cond_here) * (volt_here - volt_prev)
        above_flux = harmonic_mean(cond_here, cond_next) * (volt_next - volt_here)
        row_terms = below_flux - above_flux
        col_terms = open_terms(volt_here, cond_here, 0)
        depth_terms = open_terms(volt_here, cond_here, 1)
        diode_part = nonlinear_row(volt_here, picker(diode_field, row_index), synthesis, analysis)
        residual = row_terms + col_terms + depth_terms + picker(capacity, row_index) * time_derivative(volt_here) + diode_part - picker(drive_field, row_index)
        return (residual, lax.optimization_barrier(jnp.sum(residual * residual, axis=(0, 1))))
    residual, row_squares = lax.map(one_row, jnp.arange(NX, dtype=jnp.int32))
    summed = lax.optimization_barrier(jnp.sum(row_squares, axis=0))
    norms_out = jnp.sqrt(summed / (NX * NY * NZ) + norm_eps)
    return (residual.reshape(NX, NY, NZ * KC), norms_out)
```

```python
import functools
import math

import jax
import jax.numpy as jnp
import numpy as np
from jax import lax
from jax.experimental import pallas as pl
from jax.experimental.pallas import tpu as pltpu
from jax.sharding import PartitionSpec as P

NZ = 32
H = 32
KC = 64
S = 256
LANES = 128
TILES = NZ * KC // LANES
CHUNK = 8

base_freq = 0.1
norm_eps = 1e-06


def tables():
    orders = np.arange(1, H + 1, dtype=np.float64)
    angles = orders[:, None] * (2.0 * math.pi * np.arange(S) / S)[None, :]
    synthesis = np.concatenate([np.cos(angles), np.sin(angles)], axis=0)
    analysis = synthesis.T * (2.0 / S)
    derived = np.concatenate(
        [base_freq * orders * analysis[:, H:], -base_freq * orders * analysis[:, :H]], axis=1
    )

    def split(table):
        high = table.astype(jnp.bfloat16)
        low = (table - high.astype(np.float64)).astype(jnp.bfloat16)
        return high, low

    high, low = split(synthesis)
    forward = np.concatenate([high, high, low, low], axis=0)
    cell = 0.5 * np.concatenate([analysis, derived], axis=0)
    both = np.zeros((4 * S, LANES))
    both[: 2 * S, :KC] = cell
    both[2 * S :, KC:] = cell
    high, low = split(both)
    return jnp.asarray(forward), jnp.asarray(np.concatenate([high, low], axis=1))


def lookup(region, table, count):
    value = jnp.where(region == 0, table[0], 0.0)
    for r in range(1, count):
        value = jnp.where(region == r, table[r], value)
    return value


def harmonic_mean(left, right):
    return 2.0 * left * right / (left + right)


def spread(cells, tile, lane):
    index = 2 * tile + (lane >= KC).astype(jnp.int32)
    return jnp.take_along_axis(cells, index, axis=1, mode="promise_in_bounds")


def main_kernel(
    regions, rows, cols,
    volt_hbm, drive_ref, region_ref, mask_ref, left_ref, right_ref, sigma_ref, cap_ref,
    forward_ref, back_ref, out_ref, squares_ref,
    volt_buf, cond_buf, cell_buf, flux_buf, acc_ref, sems,
):
    i = pl.program_id(0)

    def copy(row):
        return pltpu.make_async_copy(volt_hbm.at[row], volt_buf.at[row], sems.at[row])

    @pl.when(i == 0)
    def _():
        for row in range(rows):
            copy(row).start()
        cond_buf[:, :, :NZ] = lookup(region_ref[...], sigma_ref, regions)
        acc_ref[...] = jnp.zeros_like(acc_ref)
        flux_buf[...] = jnp.zeros_like(flux_buf)
        copy(0).wait()

    @pl.when(i < rows - 1)
    def _():
        copy(i + 1).wait()

    after = jnp.minimum(i + 1, rows - 1)
    lane = lax.broadcasted_iota(jnp.int32, (cols, LANES), 1)
    col = lax.broadcasted_iota(jnp.int32, (cols, LANES), 0)
    cell_lane = lax.broadcasted_iota(jnp.int32, (cols, LANES), 1)
    cond = jnp.where(cell_lane < NZ, cond_buf[i], 1.0)
    cond_next = jnp.where(cell_lane < NZ, cond_buf[after], 1.0)
    width = NZ * KC
    edge_left = left_ref[0, :, width : width + LANES]
    edge_right = right_ref[0, :, width : width + LANES]
    g_row = jnp.where(i < rows - 1, harmonic_mean(cond, cond_next), 0.0)
    cond_after = jnp.where(
        col == cols - 1, jnp.broadcast_to(edge_right, cond.shape), pltpu.roll(cond, cols - 1, 0)
    )
    g_col = harmonic_mean(cond, cond_after)
    g_left = harmonic_mean(cond, jnp.broadcast_to(edge_left, cond.shape))
    g_depth = jnp.where(
        cell_lane < NZ - 1, harmonic_mean(cond, pltpu.roll(cond, LANES - 1, 1)), 0.0
    )
    cell_buf[0, :, :NZ] = lookup(region_ref[i], cap_ref, regions)
    cell_buf[1, :, :NZ] = mask_ref[i].astype(jnp.float32)
    capacity = cell_buf[0]
    diode = cell_buf[1]

    first = lane < KC
    half = lane % KC
    order = base_freq * (half % H + 1).astype(jnp.float32)
    order = jnp.where(half < H, order, -order)
    swap = lane ^ H

    def tile_of(ref_value, t):
        return ref_value[:, t * LANES : (t + 1) * LANES]

    turned_next = None
    prev_flux = None
    total = jnp.zeros((8, LANES), jnp.float32)
    for start in range(0, TILES, CHUNK):
        xa, xb, turned = [], [], []
        for t in range(start, start + CHUNK):
            v = volt_buf[i, :, t * LANES : (t + 1) * LANES]
            high = v.astype(jnp.bfloat16).astype(jnp.float32)
            low = v - high
            high_r = pltpu.roll(high, KC, 1)
            low_r = pltpu.roll(low, KC, 1)
            xa.append(jnp.where(first, high, low_r).astype(jnp.bfloat16))
            xb.append(jnp.where(first, high_r, low).astype(jnp.bfloat16))
            turned.append(high_r + low_r)
        if start + CHUNK < TILES:
            t = start + CHUNK
            turned.append(pltpu.roll(volt_buf[i, :, t * LANES : (t + 1) * LANES], KC, 1))
        else:
            turned.append(turned[-1])
        x = jnp.concatenate(xa + xb, axis=0)
        samples = jnp.dot(
            jnp.concatenate([x, x], axis=1), forward_ref[...], preferred_element_type=jnp.float32
        )
        size = jnp.abs(samples)
        small = jnp.exp2(size * (-2.0 / math.log(2.0)) - 1.0)
        even = (size + jnp.log(0.5 + small)).astype(jnp.bfloat16)
        charge = jnp.tanh(samples.astype(jnp.bfloat16))
        m = CHUNK * cols
        waves = jnp.concatenate([even[:m], charge[:m], even[m:], charge[m:]], axis=1)
        projected = jnp.dot(waves, back_ref[...], preferred_element_type=jnp.float32)
        projected = projected[:, :LANES] + projected[:, LANES:]
        for t in range(start, start + CHUNK):
            at = slice(t * LANES, (t + 1) * LANES)
            v = volt_buf[i, :, at]
            row_flux = spread(g_row, t, lane) * (volt_buf[after, :, at] - v)
            value = flux_buf[:, at] - row_flux
            flux_buf[:, at] = row_flux
            v_after = jnp.where(
                col == cols - 1,
                jnp.broadcast_to(right_ref[0, :, at], v.shape),
                pltpu.roll(v, cols - 1, 0),
            )
            col_flux = spread(g_col, t, lane) * (v_after - v)
            left_flux = spread(g_left[:8], t, lane[:8]) * (
                v[:8] - jnp.broadcast_to(left_ref[0, :, at], (8, LANES))
            )
            left_flux = jnp.concatenate([left_flux] * (cols // 8), axis=0)
            value += jnp.where(col == 0, left_flux, pltpu.roll(col_flux, 1, 0)) - col_flux
            v_deep = jnp.where(first, turned[t - start], turned[t - start + 1])
            deep_flux = spread(g_depth, t, lane) * (v_deep - v)
            deep_r = pltpu.roll(deep_flux, KC, 1)
            before = jnp.zeros_like(deep_r) if prev_flux is None else prev_flux
            value += jnp.where(first, before, deep_r) - deep_flux
            prev_flux = deep_r
            swapped = jnp.take_along_axis(v, swap, axis=1, mode="promise_in_bounds")
            value += spread(capacity, t, lane) * (order * swapped)
            rows_of = slice((t - start) * cols, (t - start + 1) * cols)
            value += spread(diode, t, lane) * (projected[rows_of] + 0.5 * v)
            value -= drive_ref[0, :, at]
            out_ref[0, :, at] = value
            total += jnp.sum((value * value).reshape(cols // 8, 8, LANES), axis=0)
    acc_ref[...] += total

    @pl.when(i == rows - 1)
    def _():
        squares_ref[...] = acc_ref[...]


def edge_kernel(
    last_row, width, part_ref, volt_ref, cond_ref, low_ref, high_ref, squares_ref,
    out_ref, sum_ref, acc_ref,
):
    side, step = pl.program_id(0), pl.program_id(1)

    @pl.when((side == 0) & (step == 0))
    def _():
        acc_ref[...] = squares_ref[...]

    cols = volt_ref.shape[1]
    lane = lax.broadcasted_iota(jnp.int32, (cols, LANES), 1)

    def fix(halo_ref):
        g = harmonic_mean(cond_ref[0], halo_ref[0, :, width : width + LANES])
        total = jnp.zeros((8, LANES), jnp.float32)
        for t in range(TILES):
            at = slice(t * LANES, (t + 1) * LANES)
            old = part_ref[0, :, at]
            new = old + spread(g, t, lane) * (volt_ref[0, :, at] - halo_ref[0, :, at])
            out_ref[0, :, at] = new
            change = (new - old) * (new + old)
            total += jnp.sum(change.reshape(cols // 8, 8, LANES), axis=0)
        acc_ref[...] += total

    @pl.when(side == 0)
    def _():
        fix(low_ref)

    @pl.when(side == 1)
    def _():
        fix(high_ref)

    sum_ref[...] = acc_ref[...]


def shift(block, axis, periodic):
    count = lax.axis_size(axis)
    forward = [(k, k + 1) for k in range(count - 1)]
    if periodic:
        forward.append((count - 1, 0))
    backward = [(b, a) for a, b in forward]
    return (
        lambda top: lax.ppermute(top, axis, forward),
        lambda bottom: lax.ppermute(bottom, axis, backward),
    )


def body(volt, drive, region, diode_mask, sigma_table, cap_table):
    rows, cols, width = volt.shape
    regions = sigma_table.shape[0]

    def conduct_of(part):
        onehot = part[..., None] == jnp.arange(regions, dtype=jnp.int32)
        value = jnp.sum(jnp.where(onehot, sigma_table, 0.0), axis=-1)
        return jnp.pad(value, [(0, 0)] * (value.ndim - 1) + [(0, LANES - NZ)])

    def packed(volt_part, region_part):
        return jnp.concatenate([volt_part, conduct_of(region_part)], axis=-1)

    up, down = shift(None, "gx", True)
    rightward, leftward = shift(None, "gy", False)
    left = rightward(packed(volt[:, -1:], region[:, -1:]))
    right = leftward(packed(volt[:, :1], region[:, :1]))
    low = up(packed(volt[-1:], region[-1:]))
    high = down(packed(volt[:1], region[:1]))
    forward, back = tables()

    whole = lambda *shape: pl.BlockSpec(shape, lambda i: (0,) * len(shape))
    smem = pl.BlockSpec(memory_space=pltpu.SMEM)
    row_spec = pl.BlockSpec((1, cols, width), lambda i: (i, 0, 0))
    part, squares = pl.pallas_call(
        functools.partial(main_kernel, regions, rows, cols),
        grid=(rows,),
        out_shape=(
            jax.ShapeDtypeStruct(volt.shape, jnp.float32),
            jax.ShapeDtypeStruct((8, LANES), jnp.float32),
        ),
        in_specs=[
            pl.BlockSpec(memory_space=pl.ANY),
            row_spec,
            whole(rows, cols, NZ),
            whole(rows, cols, NZ),
            pl.BlockSpec((1, 1, width + LANES), lambda i: (i, 0, 0)),
            pl.BlockSpec((1, 1, width + LANES), lambda i: (i, 0, 0)),
            smem,
            smem,
            whole(*forward.shape),
            whole(*back.shape),
        ],
        out_specs=(row_spec, whole(8, LANES)),
        scratch_shapes=[
            pltpu.VMEM((rows, cols, width), jnp.float32),
            pltpu.VMEM((rows, cols, LANES), jnp.float32),
            pltpu.VMEM((2, cols, LANES), jnp.float32),
            pltpu.VMEM((cols, width), jnp.float32),
            pltpu.VMEM((8, LANES), jnp.float32),
            pltpu.SemaphoreType.DMA((rows,)),
        ],
        compiler_params=pltpu.CompilerParams(
            dimension_semantics=("arbitrary",), vmem_limit_bytes=50 * 2**20
        ),
        cost_estimate=pl.CostEstimate(
            flops=20_000_000_000, bytes_accessed=3 * volt.size * 4, transcendentals=0
        ),
        name="cells",
    )(volt, drive, region, diode_mask, left, right, sigma_table, cap_table, forward, back)

    ends = jnp.concatenate([region[:1], region[-1:]], axis=0)
    step_cols = min(cols, 16)
    steps = cols // step_cols
    row_map = lambda s, c: (s * (rows - 1), c, 0)
    residual, sums = pl.pallas_call(
        functools.partial(edge_kernel, rows - 1, width),
        grid=(2, steps),
        out_shape=(
            jax.ShapeDtypeStruct(volt.shape, jnp.float32),
            jax.ShapeDtypeStruct((8, LANES), jnp.float32),
        ),
        in_specs=[
            pl.BlockSpec((1, step_cols, width), row_map),
            pl.BlockSpec((1, step_cols, width), row_map),
            pl.BlockSpec((1, step_cols, LANES), lambda s, c: (s, c, 0)),
            pl.BlockSpec(
                (1, step_cols, width + LANES),
                lambda s, c: (0, jnp.where(s == 0, c, steps - 1), 0),
            ),
            pl.BlockSpec(
                (1, step_cols, width + LANES), lambda s, c: (0, jnp.where(s == 1, c, 0), 0)
            ),
            pl.BlockSpec((8, LANES), lambda s, c: (0, 0)),
        ],
        out_specs=(
            pl.BlockSpec((1, step_cols, width), row_map),
            pl.BlockSpec((8, LANES), lambda s, c: (0, 0)),
        ),
        scratch_shapes=[pltpu.VMEM((8, LANES), jnp.float32)],
        input_output_aliases={0: 0},
        compiler_params=pltpu.CompilerParams(
            dimension_semantics=("arbitrary", "arbitrary"), vmem_limit_bytes=16 * 2**20
        ),
        name="edges",
    )(part, volt, conduct_of(ends), low, high, squares)

    partial_value = jnp.sum(sums.reshape(-1, KC), axis=0)
    summed = lax.psum(partial_value, ("gx", "gy"))
    cells_total = rows * cols * NZ * lax.axis_size("gx") * lax.axis_size("gy")
    return residual, jnp.sqrt(summed / cells_total + norm_eps)


def solution(mesh):
    return jax.shard_map(
        body,
        mesh=mesh,
        in_specs=(
            P("gx", "gy", None),
            P("gx", "gy", None),
            P("gx", "gy", None),
            P("gx", "gy", None),
            P(),
            P(),
        ),
        out_specs=(P("gx", "gy", None), P()),
        check_vma=False,
    )
```

```python
import functools
import math

import jax
import jax.numpy as jnp
import numpy as np
from jax import lax
from jax.experimental import pallas as pl
from jax.experimental.pallas import tpu as pltpu
from jax.sharding import PartitionSpec as P

NZ = 32
H = 32
KC = 64
S = 256
LANES = 128
TILES = NZ * KC // LANES
CHUNK = 8

base_freq = 0.1
norm_eps = 1e-06


def tables():
    orders = np.arange(1, H + 1, dtype=np.float64)
    angles = orders[:, None] * (2.0 * math.pi * np.arange(S) / S)[None, :]
    synthesis = np.concatenate([np.cos(angles), np.sin(angles)], axis=0)
    analysis = synthesis.T * (2.0 / S)
    derived = np.concatenate(
        [base_freq * orders * analysis[:, H:], -base_freq * orders * analysis[:, :H]], axis=1
    )

    def split(table):
        high = table.astype(jnp.bfloat16)
        low = (table - high.astype(np.float64)).astype(jnp.bfloat16)
        return high, low

    high, low = split(synthesis)
    forward = np.concatenate([high, high, low, low], axis=0)
    cell = 0.5 * np.concatenate([analysis, derived], axis=0)
    both = np.zeros((4 * S, LANES))
    both[: 2 * S, :KC] = cell
    both[2 * S :, KC:] = cell
    high, low = split(both)
    return jnp.asarray(forward), jnp.asarray(np.concatenate([high, low], axis=1))


def lookup(region, table, count):
    value = jnp.where(region == 0, table[0], 0.0)
    for r in range(1, count):
        value = jnp.where(region == r, table[r], value)
    return value


def harmonic_mean(left, right):
    return 2.0 * left * right / (left + right)


def spread(cells, tile, lane):
    index = 2 * tile + (lane >= KC).astype(jnp.int32)
    return jnp.take_along_axis(cells, index, axis=1, mode="promise_in_bounds")


def main_kernel(
    regions, rows, cols,
    volt_hbm, drive_ref, region_ref, mask_ref, left_ref, right_ref, sigma_ref, cap_ref,
    forward_ref, back_ref, out_ref, squares_ref,
    volt_buf, cond_buf, cell_buf, flux_buf, acc_ref, sems,
):
    i = pl.program_id(0)

    def copy(row):
        return pltpu.make_async_copy(volt_hbm.at[row], volt_buf.at[row], sems.at[row])

    @pl.when(i == 0)
    def _():
        for row in range(rows):
            copy(row).start()
        cond_buf[:, :, :NZ] = lookup(region_ref[...], sigma_ref, regions)
        acc_ref[...] = jnp.zeros_like(acc_ref)
        flux_buf[...] = jnp.zeros_like(flux_buf)
        copy(0).wait()

    @pl.when(i < rows - 1)
    def _():
        copy(i + 1).wait()

    after = jnp.minimum(i + 1, rows - 1)
    lane = lax.broadcasted_iota(jnp.int32, (cols, LANES), 1)
    col = lax.broadcasted_iota(jnp.int32, (cols, LANES), 0)
    cell_lane = lax.broadcasted_iota(jnp.int32, (cols, LANES), 1)
    cond = jnp.where(cell_lane < NZ, cond_buf[i], 1.0)
    cond_next = jnp.where(cell_lane < NZ, cond_buf[after], 1.0)
    width = NZ * KC
    edge_left = left_ref[0, :, width : width + LANES]
    edge_right = right_ref[0, :, width : width + LANES]
    g_row = jnp.where(i < rows - 1, harmonic_mean(cond, cond_next), 0.0)
    cond_after = jnp.where(
        col == cols - 1, jnp.broadcast_to(edge_right, cond.shape), pltpu.roll(cond, cols - 1, 0)
    )
    g_col = harmonic_mean(cond, cond_after)
    g_left = harmonic_mean(cond, jnp.broadcast_to(edge_left, cond.shape))
    g_depth = jnp.where(
        cell_lane < NZ - 1, harmonic_mean(cond, pltpu.roll(cond, LANES - 1, 1)), 0.0
    )
    cell_buf[0, :, :NZ] = lookup(region_ref[i], cap_ref, regions)
    cell_buf[1, :, :NZ] = mask_ref[i].astype(jnp.float32)
    capacity = cell_buf[0]
    diode = cell_buf[1]

    first = lane < KC
    half = lane % KC
    order = base_freq * (half % H + 1).astype(jnp.float32)
    order = jnp.where(half < H, order, -order)
    swap = lane ^ H

    def tile_of(ref_value, t):
        return ref_value[:, t * LANES : (t + 1) * LANES]

    turned_next = None
    prev_flux = None
    total = jnp.zeros((8, LANES), jnp.float32)
    for start in range(0, TILES, CHUNK):
        xa, xb, turned = [], [], []
        for t in range(start, start + CHUNK):
            v = volt_buf[i, :, t * LANES : (t + 1) * LANES]
            high = v.astype(jnp.bfloat16).astype(jnp.float32)
            low = v - high
            high_r = pltpu.roll(high, KC, 1)
            low_r = pltpu.roll(low, KC, 1)
            xa.append(jnp.where(first, high, low_r).astype(jnp.bfloat16))
            xb.append(jnp.where(first, high_r, low).astype(jnp.bfloat16))
            turned.append(high_r + low_r)
        if start + CHUNK < TILES:
            t = start + CHUNK
            turned.append(pltpu.roll(volt_buf[i, :, t * LANES : (t + 1) * LANES], KC, 1))
        else:
            turned.append(turned[-1])
        x = jnp.concatenate(xa + xb, axis=0)
        samples = jnp.dot(
            jnp.concatenate([x, x], axis=1), forward_ref[...], preferred_element_type=jnp.float32
        )
        size = jnp.abs(samples)
        small = jnp.exp2(size * (-2.0 / math.log(2.0)) - 1.0)
        even = (size + jnp.log(0.5 + small)).astype(jnp.bfloat16)
        charge = jnp.tanh(samples.astype(jnp.bfloat16))
        m = CHUNK * cols
        waves = jnp.concatenate([even[:m], charge[:m], even[m:], charge[m:]], axis=1)
        projected = jnp.dot(waves, back_ref[...], preferred_element_type=jnp.float32)
        projected = projected[:, :LANES] + projected[:, LANES:]
        for t in range(start, start + CHUNK):
            at = slice(t * LANES, (t + 1) * LANES)
            v = volt_buf[i, :, at]
            row_flux = spread(g_row, t, lane) * (volt_buf[after, :, at] - v)
            value = flux_buf[:, at] - row_flux
            flux_buf[:, at] = row_flux
            v_after = jnp.where(
                col == cols - 1,
                jnp.broadcast_to(right_ref[0, :, at], v.shape),
                pltpu.roll(v, cols - 1, 0),
            )
            col_flux = spread(g_col, t, lane) * (v_after - v)
            left_flux = spread(g_left[:8], t, lane[:8]) * (
                v[:8] - jnp.broadcast_to(left_ref[0, :, at], (8, LANES))
            )
            left_flux = jnp.concatenate([left_flux] * (cols // 8), axis=0)
            value += jnp.where(col == 0, left_flux, pltpu.roll(col_flux, 1, 0)) - col_flux
            v_deep = jnp.where(first, turned[t - start], turned[t - start + 1])
            deep_flux = spread(g_depth, t, lane) * (v_deep - v)
            deep_r = pltpu.roll(deep_flux, KC, 1)
            before = jnp.zeros_like(deep_r) if prev_flux is None else prev_flux
            value += jnp.where(first, before, deep_r) - deep_flux
            prev_flux = deep_r
            swapped = jnp.take_along_axis(v, swap, axis=1, mode="promise_in_bounds")
            value += spread(capacity, t, lane) * (order * swapped)
            rows_of = slice((t - start) * cols, (t - start + 1) * cols)
            value += spread(diode, t, lane) * (projected[rows_of] + 0.5 * v)
            value -= drive_ref[0, :, at]
            out_ref[0, :, at] = value
            total += jnp.sum((value * value).reshape(cols // 8, 8, LANES), axis=0)
    acc_ref[...] += total

    @pl.when(i == rows - 1)
    def _():
        squares_ref[...] = acc_ref[...]


def edge_kernel(
    last_row, width, part_ref, volt_ref, cond_ref, low_ref, high_ref, squares_ref,
    out_ref, sum_ref, acc_ref,
):
    side, step = pl.program_id(0), pl.program_id(1)

    @pl.when((side == 0) & (step == 0))
    def _():
        acc_ref[...] = squares_ref[...]

    cols = volt_ref.shape[1]
    lane = lax.broadcasted_iota(jnp.int32, (cols, LANES), 1)

    def fix(halo_ref):
        g = harmonic_mean(cond_ref[0], halo_ref[0, :, width : width + LANES])
        total = jnp.zeros((8, LANES), jnp.float32)
        for t in range(TILES):
            at = slice(t * LANES, (t + 1) * LANES)
            old = part_ref[0, :, at]
            new = old + spread(g, t, lane) * (volt_ref[0, :, at] - halo_ref[0, :, at])
            out_ref[0, :, at] = new
            change = (new - old) * (new + old)
            total += jnp.sum(change.reshape(cols // 8, 8, LANES), axis=0)
        acc_ref[...] += total

    @pl.when(side == 0)
    def _():
        fix(low_ref)

    @pl.when(side == 1)
    def _():
        fix(high_ref)

    sum_ref[...] = acc_ref[...]


def exchange(axis, count, here, got_ref, send, recv):
    def copy(peer, slot):
        return pltpu.make_async_remote_copy(
            src_ref=got_ref.at[here],
            dst_ref=got_ref.at[slot],
            send_sem=send.at[peer],
            recv_sem=recv.at[slot],
            device_id={axis: peer},
            device_id_type=pl.DeviceIdType.MESH,
        )

    peers = [lax.rem(here + d, count) for d in range(1, count)]
    for peer in peers:
        copy(peer, here).start()
    for peer in peers:
        copy(peer, peer).wait_recv()
    for peer in peers:
        copy(peer, here).wait_send()


def greet(axis, count, here):
    barrier = pltpu.get_barrier_semaphore()
    for d in range(1, count):
        pl.semaphore_signal(
            barrier,
            inc=1,
            device_id={axis: lax.rem(here + d, count)},
            device_id_type=pl.DeviceIdType.MESH,
        )


def norm_of(total, cells):
    value = jnp.broadcast_to(jnp.sum(total, axis=0, keepdims=True), total.shape)
    value = value + pltpu.roll(value, KC, 1)
    return jnp.sqrt(value / cells + norm_eps)


def reduce_kernel(nx, ny, cells, in_ref, out_ref, got_x, got_y, send_x, recv_x, send_y, recv_y):
    me_x, me_y = lax.axis_index("gx"), lax.axis_index("gy")
    greet("gx", nx, me_x)
    greet("gy", ny, me_y)
    got_x[me_x] = in_ref[...]
    pl.semaphore_wait(pltpu.get_barrier_semaphore(), nx + ny - 2)
    exchange("gx", nx, me_x, got_x, send_x, recv_x)
    got_y[me_y] = jnp.sum(got_x[...], axis=0)
    exchange("gy", ny, me_y, got_y, send_y, recv_y)
    out_ref[...] = norm_of(jnp.sum(got_y[...], axis=0), cells)


def shift(block, axis, periodic):
    count = lax.axis_size(axis)
    forward = [(k, k + 1) for k in range(count - 1)]
    if periodic:
        forward.append((count - 1, 0))
    backward = [(b, a) for a, b in forward]
    return (
        lambda top: lax.ppermute(top, axis, forward),
        lambda bottom: lax.ppermute(bottom, axis, backward),
    )


def body(volt, drive, region, diode_mask, sigma_table, cap_table):
    rows, cols, width = volt.shape
    regions = sigma_table.shape[0]

    def conduct_of(part):
        onehot = part[..., None] == jnp.arange(regions, dtype=jnp.int32)
        value = jnp.sum(jnp.where(onehot, sigma_table, 0.0), axis=-1)
        return jnp.pad(value, [(0, 0)] * (value.ndim - 1) + [(0, LANES - NZ)])

    def packed(volt_part, region_part):
        return jnp.concatenate([volt_part, conduct_of(region_part)], axis=-1)

    up, down = shift(None, "gx", True)
    rightward, leftward = shift(None, "gy", False)
    left = rightward(packed(volt[:, -1:], region[:, -1:]))
    right = leftward(packed(volt[:, :1], region[:, :1]))
    low = up(packed(volt[-1:], region[-1:]))
    high = down(packed(volt[:1], region[:1]))
    forward, back = tables()

    whole = lambda *shape: pl.BlockSpec(shape, lambda i: (0,) * len(shape))
    smem = pl.BlockSpec(memory_space=pltpu.SMEM)
    row_spec = pl.BlockSpec((1, cols, width), lambda i: (i, 0, 0))
    part, squares = pl.pallas_call(
        functools.partial(main_kernel, regions, rows, cols),
        grid=(rows,),
        out_shape=(
            jax.ShapeDtypeStruct(volt.shape, jnp.float32),
            jax.ShapeDtypeStruct((8, LANES), jnp.float32),
        ),
        in_specs=[
            pl.BlockSpec(memory_space=pl.ANY),
            row_spec,
            whole(rows, cols, NZ),
            whole(rows, cols, NZ),
            pl.BlockSpec((1, 1, width + LANES), lambda i: (i, 0, 0)),
            pl.BlockSpec((1, 1, width + LANES), lambda i: (i, 0, 0)),
            smem,
            smem,
            whole(*forward.shape),
            whole(*back.shape),
        ],
        out_specs=(row_spec, whole(8, LANES)),
        scratch_shapes=[
            pltpu.VMEM((rows, cols, width), jnp.float32),
            pltpu.VMEM((rows, cols, LANES), jnp.float32),
            pltpu.VMEM((2, cols, LANES), jnp.float32),
            pltpu.VMEM((cols, width), jnp.float32),
            pltpu.VMEM((8, LANES), jnp.float32),
            pltpu.SemaphoreType.DMA((rows,)),
        ],
        compiler_params=pltpu.CompilerParams(
            dimension_semantics=("arbitrary",), vmem_limit_bytes=50 * 2**20
        ),
        cost_estimate=pl.CostEstimate(
            flops=20_000_000_000, bytes_accessed=3 * volt.size * 4, transcendentals=0
        ),
        name="cells",
    )(volt, drive, region, diode_mask, left, right, sigma_table, cap_table, forward, back)

    ends = jnp.concatenate([region[:1], region[-1:]], axis=0)
    step_cols = min(cols, 16)
    steps = cols // step_cols
    row_map = lambda s, c: (s * (rows - 1), c, 0)
    residual, sums = pl.pallas_call(
        functools.partial(edge_kernel, rows - 1, width),
        grid=(2, steps),
        out_shape=(
            jax.ShapeDtypeStruct(volt.shape, jnp.float32),
            jax.ShapeDtypeStruct((8, LANES), jnp.float32),
        ),
        in_specs=[
            pl.BlockSpec((1, step_cols, width), row_map),
            pl.BlockSpec((1, step_cols, width), row_map),
            pl.BlockSpec((1, step_cols, LANES), lambda s, c: (s, c, 0)),
            pl.BlockSpec(
                (1, step_cols, width + LANES),
                lambda s, c: (0, jnp.where(s == 0, c, steps - 1), 0),
            ),
            pl.BlockSpec(
                (1, step_cols, width + LANES), lambda s, c: (0, jnp.where(s == 1, c, 0), 0)
            ),
            pl.BlockSpec((8, LANES), lambda s, c: (0, 0)),
        ],
        out_specs=(
            pl.BlockSpec((1, step_cols, width), row_map),
            pl.BlockSpec((8, LANES), lambda s, c: (0, 0)),
        ),
        scratch_shapes=[pltpu.VMEM((8, LANES), jnp.float32)],
        input_output_aliases={0: 0},
        compiler_params=pltpu.CompilerParams(
            dimension_semantics=("arbitrary", "arbitrary"), vmem_limit_bytes=16 * 2**20
        ),
        name="edges",
    )(part, volt, conduct_of(ends), low, high, squares)

    nx, ny = lax.axis_size("gx"), lax.axis_size("gy")
    norms = pl.pallas_call(
        functools.partial(reduce_kernel, nx, ny, float(rows * cols * NZ * nx * ny)),
        out_shape=jax.ShapeDtypeStruct((8, LANES), jnp.float32),
        in_specs=[pl.BlockSpec(memory_space=pltpu.VMEM)],
        out_specs=pl.BlockSpec(memory_space=pltpu.VMEM),
        scratch_shapes=[
            pltpu.VMEM((nx, 8, LANES), jnp.float32),
            pltpu.VMEM((ny, 8, LANES), jnp.float32),
            pltpu.SemaphoreType.DMA((nx,)),
            pltpu.SemaphoreType.DMA((nx,)),
            pltpu.SemaphoreType.DMA((ny,)),
            pltpu.SemaphoreType.DMA((ny,)),
        ],
        compiler_params=pltpu.CompilerParams(collective_id=0, has_side_effects=True),
        name="norms",
    )(sums)
    return residual, norms[0, :KC]


def solution(mesh):
    return jax.shard_map(
        body,
        mesh=mesh,
        in_specs=(
            P("gx", "gy", None),
            P("gx", "gy", None),
            P("gx", "gy", None),
            P("gx", "gy", None),
            P(),
            P(),
        ),
        out_specs=(P("gx", "gy", None), P()),
        check_vma=False,
    )
```

```python
import functools
import math

import jax
import jax.numpy as jnp
import numpy as np
from jax import lax
from jax.experimental import pallas as pl
from jax.experimental.pallas import tpu as pltpu
from jax.sharding import PartitionSpec as P

NZ = 32
H = 32
KC = 64
S = 256
LANES = 128
TILES = NZ * KC // LANES
CHUNK = 8
BLOCK = 8

base_freq = 0.1
norm_eps = 1e-06


def tables():
    orders = np.arange(1, H + 1, dtype=np.float64)
    angles = orders[:, None] * (2.0 * math.pi * np.arange(S) / S)[None, :]
    synthesis = np.concatenate([np.cos(angles), np.sin(angles)], axis=0)
    analysis = synthesis.T * (2.0 / S)
    derived = np.concatenate(
        [base_freq * orders * analysis[:, H:], -base_freq * orders * analysis[:, :H]], axis=1
    )

    def split(table):
        high = table.astype(jnp.bfloat16)
        low = (table - high.astype(np.float64)).astype(jnp.bfloat16)
        return high, low

    high, low = split(synthesis)
    forward = np.concatenate([high, high, low, low], axis=0)
    cell = 0.5 * np.concatenate([analysis, derived], axis=0)
    both = np.zeros((4 * S, LANES))
    both[: 2 * S, :KC] = cell
    both[2 * S :, KC:] = cell
    high, low = split(both)
    return jnp.asarray(forward), jnp.asarray(np.concatenate([high, low], axis=1))


def lookup(region, table, count):
    value = jnp.where(region == 0, table[0], 0.0)
    for r in range(1, count):
        value = jnp.where(region == r, table[r], value)
    return value


def harmonic_mean(left, right):
    return 2.0 * left * right / (left + right)


def spread(cells, tile, lane, base=0):
    index = base + 2 * tile + (lane >= KC).astype(jnp.int32)
    return jnp.take_along_axis(cells, index, axis=1, mode="promise_in_bounds")


def main_kernel(
    rows, cols,
    volt_hbm, low_hbm, high_hbm, drive_ref, cells_ref, low_cells, high_cells,
    left_ref, right_ref, left_cells, right_cells, forward_ref, back_ref,
    out_ref, squares_ref, volt_buf, acc_ref, sems,
):
    i = pl.program_id(0)
    sources = [low_hbm] + [volt_hbm.at[row] for row in range(rows)] + [high_hbm]

    def copy(slot):
        return pltpu.make_async_copy(sources[slot], volt_buf.at[slot], sems.at[slot])

    @pl.when(i == 0)
    def _():
        for slot in range(rows + 2):
            copy(slot).start()
        acc_ref[...] = jnp.zeros_like(acc_ref)
        copy(0).wait()
        copy(1).wait()

    for slot in range(2, rows + 2):

        @pl.when(i == slot - 2)
        def _():
            copy(slot).wait()

    lane = lax.broadcasted_iota(jnp.int32, (cols, LANES), 1)
    col = lax.broadcasted_iota(jnp.int32, (cols, LANES), 0)
    cells = cells_ref[i]
    prev_cells = jnp.where(i > 0, cells_ref[jnp.maximum(i - 1, 0)], low_cells[...])
    next_cells = jnp.where(
        i < rows - 1, cells_ref[jnp.minimum(i + 1, rows - 1)], high_cells[...]
    )
    me, count = lax.axis_index("gy"), lax.axis_size("gy")
    has_left, has_right = me > 0, me < count - 1
    g_low = harmonic_mean(cells, prev_cells)
    g_high = harmonic_mean(cells, next_cells)
    edge_left = jnp.where(has_left, left_cells[0, BLOCK - 1 :, :], 0.0)
    edge_right = jnp.where(has_right, right_cells[0, :1, :], 0.0)
    cells_after = jnp.where(
        col == cols - 1, jnp.broadcast_to(edge_right, cells.shape), pltpu.roll(cells, cols - 1, 0)
    )
    g_col = harmonic_mean(cells, cells_after)
    g_left = harmonic_mean(cells[:8], jnp.broadcast_to(edge_left, (8, LANES)))
    g_depth = jnp.where(
        lane < NZ - 1, harmonic_mean(cells, pltpu.roll(cells, LANES - 1, 1)), 0.0
    )

    first = lane < KC
    half = lane % KC
    order = base_freq * (half % H + 1).astype(jnp.float32)
    order = jnp.where(half < H, order, -order)
    swap = lane ^ H

    prev_flux = None
    total = jnp.zeros((8, LANES), jnp.float32)
    for start in range(0, TILES, CHUNK):
        xa, xb, turned = [], [], []
        for t in range(start, start + CHUNK):
            v = volt_buf[i + 1, :, t * LANES : (t + 1) * LANES]
            high = v.astype(jnp.bfloat16).astype(jnp.float32)
            low = v - high
            high_r = pltpu.roll(high, KC, 1)
            low_r = pltpu.roll(low, KC, 1)
            xa.append(jnp.where(first, high, low_r).astype(jnp.bfloat16))
            xb.append(jnp.where(first, high_r, low).astype(jnp.bfloat16))
            turned.append(high_r + low_r)
        if start + CHUNK < TILES:
            t = start + CHUNK
            turned.append(pltpu.roll(volt_buf[i + 1, :, t * LANES : (t + 1) * LANES], KC, 1))
        else:
            turned.append(turned[-1])
        x = jnp.concatenate(xa + xb, axis=0)
        samples = jnp.dot(
            jnp.concatenate([x, x], axis=1), forward_ref[...], preferred_element_type=jnp.float32
        )
        size = jnp.abs(samples)
        small = jnp.exp2(size * (-2.0 / math.log(2.0)) - 1.0)
        even = (size + jnp.log(0.5 + small)).astype(jnp.bfloat16)
        charge = jnp.tanh(samples.astype(jnp.bfloat16))
        m = CHUNK * cols
        waves = jnp.concatenate([even[:m], charge[:m], even[m:], charge[m:]], axis=1)
        projected = jnp.dot(waves, back_ref[...], preferred_element_type=jnp.float32)
        projected = projected[:, :LANES] + projected[:, LANES:]
        for t in range(start, start + CHUNK):
            at = slice(t * LANES, (t + 1) * LANES)
            v = volt_buf[i + 1, :, at]
            value = spread(g_low, t, lane) * (v - volt_buf[i, :, at])
            value -= spread(g_high, t, lane) * (volt_buf[i + 2, :, at] - v)
            right = jnp.where(has_right, right_ref[0, :1, at], 0.0)
            v_after = jnp.where(
                col == cols - 1, jnp.broadcast_to(right, v.shape), pltpu.roll(v, cols - 1, 0)
            )
            col_flux = spread(g_col, t, lane) * (v_after - v)
            left = jnp.where(has_left, left_ref[0, BLOCK - 1 :, at], 0.0)
            left_flux = spread(g_left, t, lane[:8]) * (v[:8] - jnp.broadcast_to(left, (8, LANES)))
            left_flux = jnp.concatenate([left_flux] * (cols // 8), axis=0)
            value += jnp.where(col == 0, left_flux, pltpu.roll(col_flux, 1, 0)) - col_flux
            v_deep = jnp.where(first, turned[t - start], turned[t - start + 1])
            deep_flux = spread(g_depth, t, lane) * (v_deep - v)
            deep_r = pltpu.roll(deep_flux, KC, 1)
            before = jnp.zeros_like(deep_r) if prev_flux is None else prev_flux
            value += jnp.where(first, before, deep_r) - deep_flux
            prev_flux = deep_r
            swapped = jnp.take_along_axis(v, swap, axis=1, mode="promise_in_bounds")
            value += spread(cells, t, lane, NZ) * (order * swapped)
            rows_of = slice((t - start) * cols, (t - start + 1) * cols)
            value += spread(cells, t, lane, 2 * NZ) * (projected[rows_of] + 0.5 * v)
            value -= drive_ref[0, :, at]
            out_ref[0, :, at] = value
            total += jnp.sum((value * value).reshape(cols // 8, 8, LANES), axis=0)
    acc_ref[...] += total

    @pl.when(i == rows - 1)
    def _():
        squares_ref[...] = acc_ref[...]


def exchange(axis, count, here, got_ref, send, recv):
    def copy(peer, slot):
        return pltpu.make_async_remote_copy(
            src_ref=got_ref.at[here],
            dst_ref=got_ref.at[slot],
            send_sem=send.at[peer],
            recv_sem=recv.at[slot],
            device_id={axis: peer},
            device_id_type=pl.DeviceIdType.MESH,
        )

    peers = [lax.rem(here + d, count) for d in range(1, count)]
    for peer in peers:
        copy(peer, here).start()
    for peer in peers:
        copy(peer, peer).wait_recv()
    for peer in peers:
        copy(peer, here).wait_send()


def greet(axis, count, here):
    barrier = pltpu.get_barrier_semaphore()
    for d in range(1, count):
        pl.semaphore_signal(
            barrier,
            inc=1,
            device_id={axis: lax.rem(here + d, count)},
            device_id_type=pl.DeviceIdType.MESH,
        )


def norm_of(total, cells):
    value = jnp.broadcast_to(jnp.sum(total, axis=0, keepdims=True), total.shape)
    value = value + pltpu.roll(value, KC, 1)
    return jnp.sqrt(value / cells + norm_eps)


def reduce_kernel(nx, ny, cells, in_ref, out_ref, got_x, got_y, send_x, recv_x, send_y, recv_y):
    me_x, me_y = lax.axis_index("gx"), lax.axis_index("gy")
    greet("gx", nx, me_x)
    greet("gy", ny, me_y)
    got_x[me_x] = in_ref[...]
    pl.semaphore_wait(pltpu.get_barrier_semaphore(), nx + ny - 2)
    exchange("gx", nx, me_x, got_x, send_x, recv_x)
    got_y[me_y] = jnp.sum(got_x[...], axis=0)
    exchange("gy", ny, me_y, got_y, send_y, recv_y)
    out_ref[...] = norm_of(jnp.sum(got_y[...], axis=0), cells)


def halo_kernel(
    nx, ny, rows, cols, volt, cells,
    low, low_cells, high, high_cells, left, left_cells, right, right_cells, send, recv,
):
    me_x, me_y = lax.axis_index("gx"), lax.axis_index("gy")
    up, down = lax.rem(me_x + 1, nx), lax.rem(me_x + nx - 1, nx)
    barrier = pltpu.get_barrier_semaphore()
    mesh_ids = pl.DeviceIdType.MESH

    def copy(k, source, target, axis, peer):
        return pltpu.make_async_remote_copy(
            src_ref=source, dst_ref=target, send_sem=send.at[k], recv_sem=recv.at[k],
            device_id={axis: peer}, device_id_type=mesh_ids,
        )

    first, final = pl.ds(0, BLOCK), pl.ds(cols - BLOCK, BLOCK)
    row_copies = [
        copy(0, volt.at[rows - 1], low, "gx", up),
        copy(1, volt.at[0], high, "gx", down),
        copy(2, cells.at[rows - 1], low_cells, "gx", up),
        copy(3, cells.at[0], high_cells, "gx", down),
    ]
    to_right = [
        copy(4, volt.at[:, final, :], left, "gy", me_y + 1),
        copy(5, cells.at[:, final, :], left_cells, "gy", me_y + 1),
    ]
    to_left = [
        copy(6, volt.at[:, first, :], right, "gy", me_y - 1),
        copy(7, cells.at[:, first, :], right_cells, "gy", me_y - 1),
    ]
    has_left, has_right = me_y > 0, me_y < ny - 1

    pl.semaphore_signal(barrier, inc=1, device_id={"gx": up}, device_id_type=mesh_ids)
    pl.semaphore_signal(barrier, inc=1, device_id={"gx": down}, device_id_type=mesh_ids)

    @pl.when(has_right)
    def _():
        pl.semaphore_signal(barrier, inc=1, device_id={"gy": me_y + 1}, device_id_type=mesh_ids)

    @pl.when(has_left)
    def _():
        pl.semaphore_signal(barrier, inc=1, device_id={"gy": me_y - 1}, device_id_type=mesh_ids)

    greeted = 2 + jnp.where(has_right, 1, 0) + jnp.where(has_left, 1, 0)
    pl.semaphore_wait(barrier, greeted)

    for c in row_copies:
        c.start()

    @pl.when(has_right)
    def _():
        for c in to_right:
            c.start()

    @pl.when(has_left)
    def _():
        for c in to_left:
            c.start()

    for c in row_copies:
        c.wait_recv()
        c.wait_send()

    @pl.when(has_right)
    def _():
        for c in to_right:
            c.wait_send()
        for c in to_left:
            c.wait_recv()

    @pl.when(has_left)
    def _():
        for c in to_left:
            c.wait_send()
        for c in to_right:
            c.wait_recv()


def body(volt, drive, region, diode_mask, sigma_table, cap_table):
    rows, cols, width = volt.shape
    regions = sigma_table.shape[0]
    nx, ny = lax.axis_size("gx"), lax.axis_size("gy")
    cells = jnp.concatenate(
        [
            lookup(region, sigma_table, regions),
            lookup(region, cap_table, regions),
            diode_mask.astype(jnp.float32),
            jnp.zeros((rows, cols, LANES - 3 * NZ), jnp.float32),
        ],
        axis=2,
    )
    anywhere = pl.BlockSpec(memory_space=pl.ANY)
    shaped = lambda *shape: jax.ShapeDtypeStruct(shape, jnp.float32)
    sides = (shaped(rows, BLOCK, width), shaped(rows, BLOCK, LANES))
    ends = (shaped(cols, width), shaped(cols, LANES))
    low, low_cells, high, high_cells, left, left_cells, right, right_cells = pl.pallas_call(
        functools.partial(halo_kernel, nx, ny, rows, cols),
        out_shape=ends * 2 + sides * 2,
        in_specs=[anywhere] * 2,
        out_specs=(anywhere,) * 8,
        scratch_shapes=[pltpu.SemaphoreType.DMA((8,)), pltpu.SemaphoreType.DMA((8,))],
        compiler_params=pltpu.CompilerParams(collective_id=1, has_side_effects=True),
        name="halos",
    )(volt, cells)
    forward, back = tables()

    whole = lambda *shape: pl.BlockSpec(shape, lambda i: (0,) * len(shape))
    row_spec = pl.BlockSpec((1, cols, width), lambda i: (i, 0, 0))
    side_spec = pl.BlockSpec((1, BLOCK, width), lambda i: (i, 0, 0))
    side_cells = pl.BlockSpec((1, BLOCK, LANES), lambda i: (i, 0, 0))
    residual, sums = pl.pallas_call(
        functools.partial(main_kernel, rows, cols),
        grid=(rows,),
        out_shape=(shaped(*volt.shape), shaped(8, LANES)),
        in_specs=[
            anywhere,
            anywhere,
            anywhere,
            row_spec,
            whole(rows, cols, LANES),
            whole(cols, LANES),
            whole(cols, LANES),
            side_spec,
            side_spec,
            side_cells,
            side_cells,
            whole(*forward.shape),
            whole(*back.shape),
        ],
        out_specs=(row_spec, whole(8, LANES)),
        scratch_shapes=[
            pltpu.VMEM((rows + 2, cols, width), jnp.float32),
            pltpu.VMEM((8, LANES), jnp.float32),
            pltpu.SemaphoreType.DMA((rows + 2,)),
        ],
        compiler_params=pltpu.CompilerParams(
            dimension_semantics=("arbitrary",), vmem_limit_bytes=50 * 2**20
        ),
        name="cells",
    )(
        volt, low, high, drive, cells, low_cells, high_cells,
        left, right, left_cells, right_cells, forward, back,
    )

    norms = pl.pallas_call(
        functools.partial(reduce_kernel, nx, ny, float(rows * cols * NZ * nx * ny)),
        out_shape=jax.ShapeDtypeStruct((8, LANES), jnp.float32),
        in_specs=[pl.BlockSpec(memory_space=pltpu.VMEM)],
        out_specs=pl.BlockSpec(memory_space=pltpu.VMEM),
        scratch_shapes=[
            pltpu.VMEM((nx, 8, LANES), jnp.float32),
            pltpu.VMEM((ny, 8, LANES), jnp.float32),
            pltpu.SemaphoreType.DMA((nx,)),
            pltpu.SemaphoreType.DMA((nx,)),
            pltpu.SemaphoreType.DMA((ny,)),
            pltpu.SemaphoreType.DMA((ny,)),
        ],
        compiler_params=pltpu.CompilerParams(collective_id=0, has_side_effects=True),
        name="norms",
    )(sums)
    return residual, norms[0, :KC]


def solution(mesh):
    return jax.shard_map(
        body,
        mesh=mesh,
        in_specs=(
            P("gx", "gy", None),
            P("gx", "gy", None),
            P("gx", "gy", None),
            P("gx", "gy", None),
            P(),
            P(),
        ),
        out_specs=(P("gx", "gy", None), P()),
        check_vma=False,
    )
```

```python
import functools
import math

import jax
import jax.numpy as jnp
import numpy as np
from jax import lax
from jax.experimental import pallas as pl
from jax.experimental.pallas import tpu as pltpu
from jax.sharding import PartitionSpec as P

NZ = 32
H = 32
KC = 64
S = 256
LANES = 128
TILES = NZ * KC // LANES
CHUNK = 8

base_freq = 0.1
norm_eps = 1e-06


def tables():
    orders = np.arange(1, H + 1, dtype=np.float64)
    angles = orders[:, None] * (2.0 * math.pi * np.arange(S) / S)[None, :]
    synthesis = np.concatenate([np.cos(angles), np.sin(angles)], axis=0)
    analysis = synthesis.T * (2.0 / S)
    derived = np.concatenate(
        [base_freq * orders * analysis[:, H:], -base_freq * orders * analysis[:, :H]], axis=1
    )

    def split(table):
        high = table.astype(jnp.bfloat16)
        low = (table - high.astype(np.float64)).astype(jnp.bfloat16)
        return high, low

    high, low = split(synthesis)
    forward = np.concatenate([high, high, low, low], axis=0)
    cell = 0.5 * np.concatenate([analysis, derived], axis=0)
    both = np.zeros((4 * S, LANES))
    both[: 2 * S, :KC] = cell
    both[2 * S :, KC:] = cell
    high, low = split(both)
    return jnp.asarray(forward), jnp.asarray(np.concatenate([high, low], axis=1))


def lookup(region, table, count):
    value = jnp.where(region == 0, table[0], 0.0)
    for r in range(1, count):
        value = jnp.where(region == r, table[r], value)
    return value


def harmonic_mean(left, right):
    return 2.0 * left * right / (left + right)


def spread(cells, tile, lane):
    index = 2 * tile + (lane >= KC).astype(jnp.int32)
    return jnp.take_along_axis(cells, index, axis=1, mode="promise_in_bounds")


def main_kernel(
    rows, cols, regions,
    volt_hbm, ends_hbm, drive_ref, region_ref, mask_ref, end_regions,
    side_ref, side_regions, sigma_ref, cap_ref, forward_ref, back_ref,
    out_ref, squares_ref, volt_buf, cond_buf, cell_buf, side_buf, acc_ref, sems,
):
    i = pl.program_id(0)
    sources = [ends_hbm.at[0]] + [volt_hbm.at[row] for row in range(rows)] + [ends_hbm.at[1]]

    def copy(slot):
        return pltpu.make_async_copy(sources[slot], volt_buf.at[slot], sems.at[slot])

    @pl.when(i == 0)
    def _():
        for slot in range(rows + 2):
            copy(slot).start()
        acc_ref[...] = jnp.zeros_like(acc_ref)
        cond_buf[1 : rows + 1, :, :NZ] = lookup(region_ref[...], sigma_ref, regions)
        cond_buf[0, :, :NZ] = lookup(end_regions[0], sigma_ref, regions)
        cond_buf[rows + 1, :, :NZ] = lookup(end_regions[1], sigma_ref, regions)
        copy(0).wait()
        copy(1).wait()

    for slot in range(2, rows + 2):

        @pl.when(i == slot - 2)
        def _():
            copy(slot).wait()

    lane = lax.broadcasted_iota(jnp.int32, (cols, LANES), 1)
    col = lax.broadcasted_iota(jnp.int32, (cols, LANES), 0)
    cell_buf[0, :, :NZ] = lookup(region_ref[i], cap_ref, regions)
    cell_buf[1, :, :NZ] = mask_ref[i].astype(jnp.float32)
    side_buf[0, :1, :NZ] = lookup(side_regions[0, 0], sigma_ref, regions)
    side_buf[1, :1, :NZ] = lookup(side_regions[1, 0], sigma_ref, regions)
    capacity, diode = cell_buf[0], cell_buf[1]
    cells = cond_buf[i + 1]
    me, count = lax.axis_index("gy"), lax.axis_size("gy")
    has_left, has_right = me > 0, me < count - 1
    g_low = harmonic_mean(cells, cond_buf[i])
    g_high = harmonic_mean(cells, cond_buf[i + 2])
    edge_left = jnp.where(has_left, side_buf[0, :1], 0.0)
    edge_right = jnp.where(has_right, side_buf[1, :1], 0.0)
    cells_after = jnp.where(
        col == cols - 1, jnp.broadcast_to(edge_right, cells.shape), pltpu.roll(cells, cols - 1, 0)
    )
    g_col = harmonic_mean(cells, cells_after)
    g_left = harmonic_mean(cells[:8], jnp.broadcast_to(edge_left, (8, LANES)))
    g_depth = jnp.where(
        lane < NZ - 1, harmonic_mean(cells, pltpu.roll(cells, LANES - 1, 1)), 0.0
    )

    first = lane < KC
    half = lane % KC
    order = base_freq * (half % H + 1).astype(jnp.float32)
    order = jnp.where(half < H, order, -order)
    swap = lane ^ H

    prev_flux = None
    total = jnp.zeros((8, LANES), jnp.float32)
    for start in range(0, TILES, CHUNK):
        xa, xb, turned = [], [], []
        for t in range(start, start + CHUNK):
            v = volt_buf[i + 1, :, t * LANES : (t + 1) * LANES]
            high = v.astype(jnp.bfloat16).astype(jnp.float32)
            low = v - high
            high_r = pltpu.roll(high, KC, 1)
            low_r = pltpu.roll(low, KC, 1)
            xa.append(jnp.where(first, high, low_r).astype(jnp.bfloat16))
            xb.append(jnp.where(first, high_r, low).astype(jnp.bfloat16))
            turned.append(high_r + low_r)
        if start + CHUNK < TILES:
            t = start + CHUNK
            turned.append(pltpu.roll(volt_buf[i + 1, :, t * LANES : (t + 1) * LANES], KC, 1))
        else:
            turned.append(turned[-1])
        x = jnp.concatenate(xa + xb, axis=0)
        samples = jnp.dot(
            jnp.concatenate([x, x], axis=1), forward_ref[...], preferred_element_type=jnp.float32
        )
        size = jnp.abs(samples)
        small = jnp.exp2(size * (-2.0 / math.log(2.0)) - 1.0)
        even = (size + jnp.log(0.5 + small)).astype(jnp.bfloat16)
        charge = jnp.tanh(samples.astype(jnp.bfloat16))
        m = CHUNK * cols
        waves = jnp.concatenate([even[:m], charge[:m], even[m:], charge[m:]], axis=1)
        projected = jnp.dot(waves, back_ref[...], preferred_element_type=jnp.float32)
        projected = projected[:, :LANES] + projected[:, LANES:]
        for t in range(start, start + CHUNK):
            at = slice(t * LANES, (t + 1) * LANES)
            v = volt_buf[i + 1, :, at]
            value = spread(g_low, t, lane) * (v - volt_buf[i, :, at])
            value -= spread(g_high, t, lane) * (volt_buf[i + 2, :, at] - v)
            right = jnp.where(has_right, side_ref[1, 0, :, at], 0.0)
            v_after = jnp.where(
                col == cols - 1, jnp.broadcast_to(right, v.shape), pltpu.roll(v, cols - 1, 0)
            )
            col_flux = spread(g_col, t, lane) * (v_after - v)
            left = jnp.where(has_left, side_ref[0, 0, :, at], 0.0)
            left_flux = spread(g_left, t, lane[:8]) * (v[:8] - jnp.broadcast_to(left, (8, LANES)))
            left_flux = jnp.concatenate([left_flux] * (cols // 8), axis=0)
            value += jnp.where(col == 0, left_flux, pltpu.roll(col_flux, 1, 0)) - col_flux
            v_deep = jnp.where(first, turned[t - start], turned[t - start + 1])
            deep_flux = spread(g_depth, t, lane) * (v_deep - v)
            deep_r = pltpu.roll(deep_flux, KC, 1)
            before = jnp.zeros_like(deep_r) if prev_flux is None else prev_flux
            value += jnp.where(first, before, deep_r) - deep_flux
            prev_flux = deep_r
            swapped = jnp.take_along_axis(v, swap, axis=1, mode="promise_in_bounds")
            value += spread(capacity, t, lane) * (order * swapped)
            rows_of = slice((t - start) * cols, (t - start + 1) * cols)
            value += spread(diode, t, lane) * (projected[rows_of] + 0.5 * v)
            value -= drive_ref[0, :, at]
            out_ref[0, :, at] = value
            total += jnp.sum((value * value).reshape(cols // 8, 8, LANES), axis=0)
    acc_ref[...] += total

    @pl.when(i == rows - 1)
    def _():
        squares_ref[...] = acc_ref[...]


def exchange(axis, count, here, got_ref, send, recv):
    def copy(peer, slot):
        return pltpu.make_async_remote_copy(
            src_ref=got_ref.at[here],
            dst_ref=got_ref.at[slot],
            send_sem=send.at[peer],
            recv_sem=recv.at[slot],
            device_id={axis: peer},
            device_id_type=pl.DeviceIdType.MESH,
        )

    peers = [lax.rem(here + d, count) for d in range(1, count)]
    for peer in peers:
        copy(peer, here).start()
    for peer in peers:
        copy(peer, peer).wait_recv()
    for peer in peers:
        copy(peer, here).wait_send()


def greet(axis, count, here):
    barrier = pltpu.get_barrier_semaphore()
    for d in range(1, count):
        pl.semaphore_signal(
            barrier,
            inc=1,
            device_id={axis: lax.rem(here + d, count)},
            device_id_type=pl.DeviceIdType.MESH,
        )


def norm_of(total, cells):
    value = jnp.broadcast_to(jnp.sum(total, axis=0, keepdims=True), total.shape)
    value = value + pltpu.roll(value, KC, 1)
    return jnp.sqrt(value / cells + norm_eps)


def reduce_kernel(nx, ny, cells, in_ref, out_ref, got_x, got_y, send_x, recv_x, send_y, recv_y):
    me_x, me_y = lax.axis_index("gx"), lax.axis_index("gy")
    greet("gx", nx, me_x)
    greet("gy", ny, me_y)
    got_x[me_x] = in_ref[...]
    pl.semaphore_wait(pltpu.get_barrier_semaphore(), nx + ny - 2)
    exchange("gx", nx, me_x, got_x, send_x, recv_x)
    got_y[me_y] = jnp.sum(got_x[...], axis=0)
    exchange("gy", ny, me_y, got_y, send_y, recv_y)
    out_ref[...] = norm_of(jnp.sum(got_y[...], axis=0), cells)


def halo_kernel(
    nx, ny, rows, cols, volt, region, ends, end_regions, sides, side_regions, send, recv,
):
    me_x, me_y = lax.axis_index("gx"), lax.axis_index("gy")
    up, down = lax.rem(me_x + 1, nx), lax.rem(me_x + nx - 1, nx)
    barrier = pltpu.get_barrier_semaphore()
    mesh_ids = pl.DeviceIdType.MESH

    def copy(k, source, target, axis, peer):
        return pltpu.make_async_remote_copy(
            src_ref=source, dst_ref=target, send_sem=send.at[k], recv_sem=recv.at[k],
            device_id={axis: peer}, device_id_type=mesh_ids,
        )

    first, final = pl.ds(0, 1), pl.ds(cols - 1, 1)
    row_copies = [
        copy(0, volt.at[rows - 1], ends.at[0], "gx", up),
        copy(1, volt.at[0], ends.at[1], "gx", down),
        copy(2, region.at[rows - 1], end_regions.at[0], "gx", up),
        copy(3, region.at[0], end_regions.at[1], "gx", down),
    ]
    to_right = [
        copy(4, volt.at[:, final, :], sides.at[0], "gy", me_y + 1),
        copy(5, region.at[:, final, :], side_regions.at[0], "gy", me_y + 1),
    ]
    to_left = [
        copy(6, volt.at[:, first, :], sides.at[1], "gy", me_y - 1),
        copy(7, region.at[:, first, :], side_regions.at[1], "gy", me_y - 1),
    ]
    has_left, has_right = me_y > 0, me_y < ny - 1

    pl.semaphore_signal(barrier, inc=1, device_id={"gx": up}, device_id_type=mesh_ids)
    pl.semaphore_signal(barrier, inc=1, device_id={"gx": down}, device_id_type=mesh_ids)

    @pl.when(has_right)
    def _():
        pl.semaphore_signal(barrier, inc=1, device_id={"gy": me_y + 1}, device_id_type=mesh_ids)

    @pl.when(has_left)
    def _():
        pl.semaphore_signal(barrier, inc=1, device_id={"gy": me_y - 1}, device_id_type=mesh_ids)

    greeted = 2 + jnp.where(has_right, 1, 0) + jnp.where(has_left, 1, 0)
    pl.semaphore_wait(barrier, greeted)

    for c in row_copies:
        c.start()

    @pl.when(has_right)
    def _():
        for c in to_right:
            c.start()

    @pl.when(has_left)
    def _():
        for c in to_left:
            c.start()

    for c in row_copies:
        c.wait_recv()
        c.wait_send()

    @pl.when(has_right)
    def _():
        for c in to_right:
            c.wait_send()
        for c in to_left:
            c.wait_recv()

    @pl.when(has_left)
    def _():
        for c in to_left:
            c.wait_send()
        for c in to_right:
            c.wait_recv()


def body(volt, drive, region, diode_mask, sigma_table, cap_table):
    rows, cols, width = volt.shape
    regions = sigma_table.shape[0]
    nx, ny = lax.axis_size("gx"), lax.axis_size("gy")
    anywhere = pl.BlockSpec(memory_space=pl.ANY)
    shaped = lambda *shape: jax.ShapeDtypeStruct(shape, jnp.float32)
    ends, end_regions, sides, side_regions = pl.pallas_call(
        functools.partial(halo_kernel, nx, ny, rows, cols),
        out_shape=(
            shaped(2, cols, width),
            jax.ShapeDtypeStruct((2, cols, NZ), jnp.int32),
            shaped(2, rows, 1, width),
            jax.ShapeDtypeStruct((2, rows, 1, NZ), jnp.int32),
        ),
        in_specs=[anywhere] * 2,
        out_specs=(anywhere,) * 4,
        scratch_shapes=[pltpu.SemaphoreType.DMA((8,)), pltpu.SemaphoreType.DMA((8,))],
        compiler_params=pltpu.CompilerParams(collective_id=1, has_side_effects=True),
        name="halos",
    )(volt, region)
    forward, back = tables()

    whole = lambda *shape: pl.BlockSpec(shape, lambda i: (0,) * len(shape))
    row_spec = pl.BlockSpec((1, cols, width), lambda i: (i, 0, 0))
    side_map = lambda i: (0, i, 0, 0)
    smem = pl.BlockSpec(memory_space=pltpu.SMEM)
    residual, sums = pl.pallas_call(
        functools.partial(main_kernel, rows, cols, regions),
        grid=(rows,),
        out_shape=(shaped(*volt.shape), shaped(8, LANES)),
        in_specs=[
            anywhere,
            anywhere,
            row_spec,
            whole(rows, cols, NZ),
            whole(rows, cols, NZ),
            whole(2, cols, NZ),
            pl.BlockSpec((2, 1, 1, width), side_map),
            pl.BlockSpec((2, 1, 1, NZ), side_map),
            smem,
            smem,
            whole(*forward.shape),
            whole(*back.shape),
        ],
        out_specs=(row_spec, whole(8, LANES)),
        scratch_shapes=[
            pltpu.VMEM((rows + 2, cols, width), jnp.float32),
            pltpu.VMEM((rows + 2, cols, LANES), jnp.float32),
            pltpu.VMEM((2, cols, LANES), jnp.float32),
            pltpu.VMEM((2, 8, LANES), jnp.float32),
            pltpu.VMEM((8, LANES), jnp.float32),
            pltpu.SemaphoreType.DMA((rows + 2,)),
        ],
        compiler_params=pltpu.CompilerParams(
            dimension_semantics=("arbitrary",), vmem_limit_bytes=50 * 2**20
        ),
        name="cells",
    )(
        volt, ends, drive, region, diode_mask, end_regions, sides, side_regions,
        sigma_table, cap_table, forward, back,
    )

    norms = pl.pallas_call(
        functools.partial(reduce_kernel, nx, ny, float(rows * cols * NZ * nx * ny)),
        out_shape=jax.ShapeDtypeStruct((8, LANES), jnp.float32),
        in_specs=[pl.BlockSpec(memory_space=pltpu.VMEM)],
        out_specs=pl.BlockSpec(memory_space=pltpu.VMEM),
        scratch_shapes=[
            pltpu.VMEM((nx, 8, LANES), jnp.float32),
            pltpu.VMEM((ny, 8, LANES), jnp.float32),
            pltpu.SemaphoreType.DMA((nx,)),
            pltpu.SemaphoreType.DMA((nx,)),
            pltpu.SemaphoreType.DMA((ny,)),
            pltpu.SemaphoreType.DMA((ny,)),
        ],
        compiler_params=pltpu.CompilerParams(collective_id=0, has_side_effects=True),
        name="norms",
    )(sums)
    return residual, norms[0, :KC]


def solution(mesh):
    return jax.shard_map(
        body,
        mesh=mesh,
        in_specs=(
            P("gx", "gy", None),
            P("gx", "gy", None),
            P("gx", "gy", None),
            P("gx", "gy", None),
            P(),
            P(),
        ),
        out_specs=(P("gx", "gy", None), P()),
        check_vma=False,
    )
```

```python
import functools
import math

import jax
import jax.numpy as jnp
import numpy as np
from jax import lax
from jax.experimental import pallas as pl
from jax.experimental.pallas import tpu as pltpu
from jax.sharding import PartitionSpec as P

NZ = 32
H = 32
KC = 64
S = 256
LANES = 128
TILES = NZ * KC // LANES
CHUNK = 8

base_freq = 0.1
norm_eps = 1e-06


def tables():
    orders = np.arange(1, H + 1, dtype=np.float64)
    angles = orders[:, None] * (2.0 * math.pi * np.arange(S) / S)[None, :]
    synthesis = np.concatenate([np.cos(angles), np.sin(angles)], axis=0)
    analysis = synthesis.T * (2.0 / S)
    derived = np.concatenate(
        [base_freq * orders * analysis[:, H:], -base_freq * orders * analysis[:, :H]], axis=1
    )

    def split(table):
        high = table.astype(jnp.bfloat16)
        low = (table - high.astype(np.float64)).astype(jnp.bfloat16)
        return high, low

    high, low = split(synthesis)
    forward = np.concatenate([high, high, low, low], axis=0)
    cell = 0.5 * np.concatenate([analysis, derived], axis=0)
    both = np.zeros((4 * S, LANES))
    both[: 2 * S, :KC] = cell
    both[2 * S :, KC:] = cell
    high, low = split(both)
    return jnp.asarray(forward), jnp.asarray(np.concatenate([high, low], axis=1))


def lookup(region, table, count):
    value = jnp.where(region == 0, table[0], 0.0)
    for r in range(1, count):
        value = jnp.where(region == r, table[r], value)
    return value


def harmonic_mean(left, right):
    return 2.0 * left * right / (left + right)


def spread(cells, tile, lane):
    index = 2 * tile + (lane >= KC).astype(jnp.int32)
    return jnp.take_along_axis(cells, index, axis=1, mode="promise_in_bounds")


def main_kernel(
    rows, cols, regions,
    volt_hbm, ends_hbm, drive_ref, region_ref, mask_ref, end_regions,
    side_ref, side_regions, sigma_ref, cap_ref, forward_ref, back_ref,
    out_ref, squares_ref, volt_buf, cond_buf, cell_buf, side_buf, acc_ref, sems,
):
    i = pl.program_id(0)
    sources = [ends_hbm.at[0]] + [volt_hbm.at[row] for row in range(rows)] + [ends_hbm.at[1]]

    def copy(slot):
        return pltpu.make_async_copy(sources[slot], volt_buf.at[slot], sems.at[slot])

    @pl.when(i == 0)
    def _():
        for slot in range(rows + 2):
            copy(slot).start()
        acc_ref[...] = jnp.zeros_like(acc_ref)
        cond_buf[1 : rows + 1, :, :NZ] = lookup(region_ref[...], sigma_ref, regions)
        cond_buf[0, :, :NZ] = lookup(end_regions[0], sigma_ref, regions)
        cond_buf[rows + 1, :, :NZ] = lookup(end_regions[1], sigma_ref, regions)
        copy(0).wait()
        copy(1).wait()

    for slot in range(2, rows + 2):

        @pl.when(i == slot - 2)
        def _():
            copy(slot).wait()

    lane = lax.broadcasted_iota(jnp.int32, (cols, LANES), 1)
    col = lax.broadcasted_iota(jnp.int32, (cols, LANES), 0)
    cell_buf[0, :, :NZ] = lookup(region_ref[i], cap_ref, regions)
    cell_buf[1, :, :NZ] = mask_ref[i].astype(jnp.float32)
    side_buf[0, :1, :NZ] = lookup(side_regions[0, 0], sigma_ref, regions)
    side_buf[1, :1, :NZ] = lookup(side_regions[1, 0], sigma_ref, regions)
    capacity, diode = cell_buf[0], cell_buf[1]
    cells = cond_buf[i + 1]
    me, count = lax.axis_index("gy"), lax.axis_size("gy")
    has_left, has_right = me > 0, me < count - 1
    g_low = harmonic_mean(cells, cond_buf[i])
    g_high = harmonic_mean(cells, cond_buf[i + 2])
    edge_left = jnp.where(has_left, side_buf[0, :1], 0.0)
    edge_right = jnp.where(has_right, side_buf[1, :1], 0.0)
    cells_after = jnp.where(
        col == cols - 1, jnp.broadcast_to(edge_right, cells.shape), pltpu.roll(cells, cols - 1, 0)
    )
    g_col = harmonic_mean(cells, cells_after)
    g_left = harmonic_mean(cells[:8], jnp.broadcast_to(edge_left, (8, LANES)))
    g_depth = jnp.where(
        lane < NZ - 1, harmonic_mean(cells, pltpu.roll(cells, LANES - 1, 1)), 0.0
    )

    first = lane < KC
    half = lane % KC
    order = base_freq * (half % H + 1).astype(jnp.float32)
    order = jnp.where(half < H, order, -order)
    swap = lane ^ H

    prev_flux = None
    total = jnp.zeros((8, LANES), jnp.float32)
    for start in range(0, TILES, CHUNK):
        xa, xb, turned = [], [], []
        for t in range(start, start + CHUNK):
            v = volt_buf[i + 1, :, t * LANES : (t + 1) * LANES]
            high = v.astype(jnp.bfloat16).astype(jnp.float32)
            low = v - high
            high_r = pltpu.roll(high, KC, 1)
            low_r = pltpu.roll(low, KC, 1)
            xa.append(jnp.where(first, high, low_r).astype(jnp.bfloat16))
            xb.append(jnp.where(first, high_r, low).astype(jnp.bfloat16))
            turned.append(high_r + low_r)
        if start + CHUNK < TILES:
            t = start + CHUNK
            turned.append(pltpu.roll(volt_buf[i + 1, :, t * LANES : (t + 1) * LANES], KC, 1))
        else:
            turned.append(turned[-1])
        x = jnp.concatenate(xa + xb, axis=0)
        samples = jnp.dot(
            jnp.concatenate([x, x], axis=1), forward_ref[...], preferred_element_type=jnp.float32
        )
        size = jnp.abs(samples)
        small = jnp.exp2(size * (-2.0 / math.log(2.0)) - 1.0)
        even = (size + jnp.log(0.5 + small)).astype(jnp.bfloat16)
        charge = jnp.tanh(samples.astype(jnp.bfloat16))
        m = CHUNK * cols
        waves = jnp.concatenate([even[:m], charge[:m], even[m:], charge[m:]], axis=1)
        projected = jnp.dot(waves, back_ref[...], preferred_element_type=jnp.float32)
        projected = projected[:, :LANES] + projected[:, LANES:]
        for t in range(start, start + CHUNK):
            at = slice(t * LANES, (t + 1) * LANES)
            v = volt_buf[i + 1, :, at]
            value = spread(g_low, t, lane) * (v - volt_buf[i, :, at])
            value -= spread(g_high, t, lane) * (volt_buf[i + 2, :, at] - v)
            right = jnp.where(has_right, side_ref[1, 0, :, at], 0.0)
            v_after = jnp.where(
                col == cols - 1, jnp.broadcast_to(right, v.shape), pltpu.roll(v, cols - 1, 0)
            )
            col_flux = spread(g_col, t, lane) * (v_after - v)
            left = jnp.where(has_left, side_ref[0, 0, :, at], 0.0)
            left_flux = spread(g_left, t, lane[:8]) * (v[:8] - jnp.broadcast_to(left, (8, LANES)))
            left_flux = jnp.concatenate([left_flux] * (cols // 8), axis=0)
            value += jnp.where(col == 0, left_flux, pltpu.roll(col_flux, 1, 0)) - col_flux
            v_deep = jnp.where(first, turned[t - start], turned[t - start + 1])
            deep_flux = spread(g_depth, t, lane) * (v_deep - v)
            deep_r = pltpu.roll(deep_flux, KC, 1)
            before = jnp.zeros_like(deep_r) if prev_flux is None else prev_flux
            value += jnp.where(first, before, deep_r) - deep_flux
            prev_flux = deep_r
            swapped = jnp.take_along_axis(v, swap, axis=1, mode="promise_in_bounds")
            value += spread(capacity, t, lane) * (order * swapped)
            rows_of = slice((t - start) * cols, (t - start + 1) * cols)
            value += spread(diode, t, lane) * (projected[rows_of] + 0.5 * v)
            value -= drive_ref[0, :, at]
            out_ref[0, :, at] = value
            total += jnp.sum((value * value).reshape(cols // 8, 8, LANES), axis=0)
    acc_ref[...] += total

    @pl.when(i == rows - 1)
    def _():
        squares_ref[...] = acc_ref[...]


def exchange(axis, count, here, got_ref, send, recv):
    def copy(peer, slot):
        return pltpu.make_async_remote_copy(
            src_ref=got_ref.at[here],
            dst_ref=got_ref.at[slot],
            send_sem=send.at[peer],
            recv_sem=recv.at[slot],
            device_id={axis: peer},
            device_id_type=pl.DeviceIdType.MESH,
        )

    peers = [lax.rem(here + d, count) for d in range(1, count)]
    for peer in peers:
        copy(peer, here).start()
    for peer in peers:
        copy(peer, peer).wait_recv()
    for peer in peers:
        copy(peer, here).wait_send()


def greet(axis, count, here):
    barrier = pltpu.get_barrier_semaphore()
    for d in range(1, count):
        pl.semaphore_signal(
            barrier,
            inc=1,
            device_id={axis: lax.rem(here + d, count)},
            device_id_type=pl.DeviceIdType.MESH,
        )


def norm_of(total, cells):
    value = jnp.broadcast_to(total, (8, LANES))
    value = value + pltpu.roll(value, KC, 1)
    return jnp.sqrt(value / cells + norm_eps)


def reduce_kernel(nx, ny, cells, in_ref, out_ref, got_x, got_y, send_x, recv_x, send_y, recv_y):
    me_x, me_y = lax.axis_index("gx"), lax.axis_index("gy")
    greet("gx", nx, me_x)
    greet("gy", ny, me_y)
    got_x[me_x] = jnp.sum(in_ref[...], axis=0, keepdims=True)
    pl.semaphore_wait(pltpu.get_barrier_semaphore(), nx + ny - 2)
    exchange("gx", nx, me_x, got_x, send_x, recv_x)
    got_y[me_y] = jnp.sum(got_x[...], axis=0)
    exchange("gy", ny, me_y, got_y, send_y, recv_y)
    out_ref[...] = norm_of(jnp.sum(got_y[...], axis=0), cells)


def halo_kernel(
    nx, ny, rows, cols, volt, region, ends, end_regions, sides, side_regions, send, recv,
):
    me_x, me_y = lax.axis_index("gx"), lax.axis_index("gy")
    up, down = lax.rem(me_x + 1, nx), lax.rem(me_x + nx - 1, nx)
    barrier = pltpu.get_barrier_semaphore()
    mesh_ids = pl.DeviceIdType.MESH

    def copy(k, source, target, axis, peer):
        return pltpu.make_async_remote_copy(
            src_ref=source, dst_ref=target, send_sem=send.at[k], recv_sem=recv.at[k],
            device_id={axis: peer}, device_id_type=mesh_ids,
        )

    first, final = pl.ds(0, 1), pl.ds(cols - 1, 1)
    row_copies = [
        copy(0, volt.at[rows - 1], ends.at[0], "gx", up),
        copy(1, volt.at[0], ends.at[1], "gx", down),
        copy(2, region.at[rows - 1], end_regions.at[0], "gx", up),
        copy(3, region.at[0], end_regions.at[1], "gx", down),
    ]
    to_right = [
        copy(4, volt.at[:, final, :], sides.at[0], "gy", me_y + 1),
        copy(5, region.at[:, final, :], side_regions.at[0], "gy", me_y + 1),
    ]
    to_left = [
        copy(6, volt.at[:, first, :], sides.at[1], "gy", me_y - 1),
        copy(7, region.at[:, first, :], side_regions.at[1], "gy", me_y - 1),
    ]
    has_left, has_right = me_y > 0, me_y < ny - 1

    pl.semaphore_signal(barrier, inc=1, device_id={"gx": up}, device_id_type=mesh_ids)
    pl.semaphore_signal(barrier, inc=1, device_id={"gx": down}, device_id_type=mesh_ids)

    @pl.when(has_right)
    def _():
        pl.semaphore_signal(barrier, inc=1, device_id={"gy": me_y + 1}, device_id_type=mesh_ids)

    @pl.when(has_left)
    def _():
        pl.semaphore_signal(barrier, inc=1, device_id={"gy": me_y - 1}, device_id_type=mesh_ids)

    greeted = 2 + jnp.where(has_right, 1, 0) + jnp.where(has_left, 1, 0)
    pl.semaphore_wait(barrier, greeted)

    for c in row_copies:
        c.start()

    @pl.when(has_right)
    def _():
        for c in to_right:
            c.start()

    @pl.when(has_left)
    def _():
        for c in to_left:
            c.start()

    for c in row_copies:
        c.wait_recv()
        c.wait_send()

    @pl.when(has_right)
    def _():
        for c in to_right:
            c.wait_send()
        for c in to_left:
            c.wait_recv()

    @pl.when(has_left)
    def _():
        for c in to_left:
            c.wait_send()
        for c in to_right:
            c.wait_recv()


def body(volt, drive, region, diode_mask, sigma_table, cap_table):
    rows, cols, width = volt.shape
    regions = sigma_table.shape[0]
    nx, ny = lax.axis_size("gx"), lax.axis_size("gy")
    anywhere = pl.BlockSpec(memory_space=pl.ANY)
    shaped = lambda *shape: jax.ShapeDtypeStruct(shape, jnp.float32)
    ends, end_regions, sides, side_regions = pl.pallas_call(
        functools.partial(halo_kernel, nx, ny, rows, cols),
        out_shape=(
            shaped(2, cols, width),
            jax.ShapeDtypeStruct((2, cols, NZ), jnp.int32),
            shaped(2, rows, 1, width),
            jax.ShapeDtypeStruct((2, rows, 1, NZ), jnp.int32),
        ),
        in_specs=[anywhere] * 2,
        out_specs=(anywhere,) * 4,
        scratch_shapes=[pltpu.SemaphoreType.DMA((8,)), pltpu.SemaphoreType.DMA((8,))],
        compiler_params=pltpu.CompilerParams(collective_id=1, has_side_effects=True),
        name="halos",
    )(volt, region)
    forward, back = tables()

    whole = lambda *shape: pl.BlockSpec(shape, lambda i: (0,) * len(shape))
    row_spec = pl.BlockSpec((1, cols, width), lambda i: (i, 0, 0))
    side_map = lambda i: (0, i, 0, 0)
    smem = pl.BlockSpec(memory_space=pltpu.SMEM)
    residual, sums = pl.pallas_call(
        functools.partial(main_kernel, rows, cols, regions),
        grid=(rows,),
        out_shape=(shaped(*volt.shape), shaped(8, LANES)),
        in_specs=[
            anywhere,
            anywhere,
            row_spec,
            whole(rows, cols, NZ),
            whole(rows, cols, NZ),
            whole(2, cols, NZ),
            pl.BlockSpec((2, 1, 1, width), side_map),
            pl.BlockSpec((2, 1, 1, NZ), side_map),
            smem,
            smem,
            whole(*forward.shape),
            whole(*back.shape),
        ],
        out_specs=(row_spec, whole(8, LANES)),
        scratch_shapes=[
            pltpu.VMEM((rows + 2, cols, width), jnp.float32),
            pltpu.VMEM((rows + 2, cols, LANES), jnp.float32),
            pltpu.VMEM((2, cols, LANES), jnp.float32),
            pltpu.VMEM((2, 8, LANES), jnp.float32),
            pltpu.VMEM((8, LANES), jnp.float32),
            pltpu.SemaphoreType.DMA((rows + 2,)),
        ],
        compiler_params=pltpu.CompilerParams(
            dimension_semantics=("arbitrary",), vmem_limit_bytes=50 * 2**20
        ),
        name="cells",
    )(
        volt, ends, drive, region, diode_mask, end_regions, sides, side_regions,
        sigma_table, cap_table, forward, back,
    )

    norms = pl.pallas_call(
        functools.partial(reduce_kernel, nx, ny, float(rows * cols * NZ * nx * ny)),
        out_shape=jax.ShapeDtypeStruct((8, LANES), jnp.float32),
        in_specs=[pl.BlockSpec(memory_space=pltpu.VMEM)],
        out_specs=pl.BlockSpec(memory_space=pltpu.VMEM),
        scratch_shapes=[
            pltpu.VMEM((nx, 1, LANES), jnp.float32),
            pltpu.VMEM((ny, 1, LANES), jnp.float32),
            pltpu.SemaphoreType.DMA((nx,)),
            pltpu.SemaphoreType.DMA((nx,)),
            pltpu.SemaphoreType.DMA((ny,)),
            pltpu.SemaphoreType.DMA((ny,)),
        ],
        compiler_params=pltpu.CompilerParams(collective_id=0, has_side_effects=True),
        name="norms",
    )(sums)
    return residual, norms[0, :KC]


def solution(mesh):
    return jax.shard_map(
        body,
        mesh=mesh,
        in_specs=(
            P("gx", "gy", None),
            P("gx", "gy", None),
            P("gx", "gy", None),
            P("gx", "gy", None),
            P(),
            P(),
        ),
        out_specs=(P("gx", "gy", None), P()),
        check_vma=False,
    )
```
